32 devices in a mesh: dp: 2 (over y), expert: 4 (over z), ffn: 4 (over x, core).
Axes of the slice: x: 2, y: 2, z: 4, core: 2. Of those that a mesh axis runs over, the one named last changes fastest.
Arguments:
- tokens: bfloat16 [64, 6144], P(('dp', 'expert'), 'ffn'), may hold values from -6 to 6
- out_grad: bfloat16 [64, 6144], P(('dp', 'expert'), 'ffn'), may hold values from -6 to 6
- expert_ids: int32 [64, 2], P(('dp', 'expert')), may hold values from 0 to 3, all different within a row; in each aligned block of 8 rows (0 to 7, 8 to 15, ...) at most 6 rows name the same one
- tenant_ids: int32 [64], P(('dp', 'expert')), may hold values from 0 to 7
- router_logits: float32 [64, 2], P(('dp', 'expert')), may hold values from -8 to 8
- gate_projection_weight: bfloat16 [4, 6144, 8192], P('expert', None, ('dp', 'ffn')), may hold values from -0.078125 to 0.078125
- up_projection_weight: bfloat16 [4, 6144, 8192], P('expert', None, ('dp', 'ffn')), may hold values from -0.078125 to 0.078125
- down_projection_weight: bfloat16 [4, 8192, 6144], P('expert', ('dp', 'ffn')), may hold values from -0.0625 to 0.0625
- input_down_maps: bfloat16 [4, 6144, 256], P('expert', 'ffn'), may hold values from -0.078125 to 0.078125
- input_up_maps: bfloat16 [4, 2, 128, 8192], P('expert', None, None, ('dp', 'ffn')), may hold values from -1.5 to 1.5
- output_down_map: bfloat16 [4, 8192, 128], P('expert', ('dp', 'ffn')), may hold values from -0.0625 to 0.0625
- output_up_map: bfloat16 [4, 128, 6144], P('expert', None, 'ffn'), may hold values from -1.5 to 1.5
Outputs:
- mixed: bfloat16 [64, 6144], P(('dp', 'expert'), 'ffn')
- input_grad: bfloat16 [64, 6144], P(('dp', 'expert'), 'ffn')
- input_down_gradient: float32 [4, 6144, 256], P('expert', 'ffn')
- input_up_gradient: float32 [4, 2, 128, 8192], P('expert', None, None, ('dp', 'ffn'))
- output_down_gradient: float32 [4, 8192, 128], P('expert', ('dp', 'ffn'))
- output_up_gradient: float32 [4, 128, 6144], P('expert', None, 'ffn')
The draws below stay inside these ranges and needn't reach their ends.
Inputs may be any that keep to these rules, and one draw needn't show every extreme that they name: `expert_ids`: each row names 2 different experts. Among the rows of one device's block of 8 tokens no expert is named more than 6 times; in some blocks one expert is named exactly 6 times.
All inputs are finite; a program needn't handle non-finite values.
Results may differ from the reference program's by a relative error of at most 0.0073.
Values may be sent and summed in bfloat16 or wider, within the bound.
A program may use at most 256 MiB of HBM per device.

```python
import math
import jax
import jax.numpy as jnp
import numpy as np
from jax import lax

D = 6144
FF = 8192
RANK = 16
TENANTS = 8
TOP = 2
TOK_DEV = 8
EXPERTS = 4
TOKENS = 64
CAP = 6
ROWS = 48
TENANT_RANKS = 128


def touch_ends(drawn, stream_key, low, largest):
    place = [jax.random.randint(jax.random.fold_in(stream_key, axis), (), 0, length) for axis, length in enumerate(drawn.shape)]
    main_axis = drawn.shape.index(max(drawn.shape))
    next_to = place[:main_axis] + [(place[main_axis] + 1) % drawn.shape[main_axis]] + place[main_axis + 1:]
    return drawn.at[tuple(place)].set(low).at[tuple(next_to)].set(largest)


def block_levels(key, dims, split, least, high):
    factor_of = 1.0
    for dim, shards_of in split:
        heights = jax.random.uniform(jax.random.fold_in(jax.random.fold_in(key, 6), dim), (shards_of,), jnp.float32, least / len(split), high / len(split))
        factor_of = factor_of * jnp.repeat(jnp.exp(heights), dims[dim] // shards_of).reshape((-1,) + (1,) * (len(dims) - 1 - dim))
    return factor_of


def routed_block(stream_key, own, number, rows, number_of, top, limit, lean):
    order = jax.random.permutation(stream_key, number_of)
    heavy_load, ordinary = shares(number_of, rows * top, limit, lean, True), shares(number_of, rows * top, limit, lean, False)
    places = jnp.arange(number_of)

    def named(tallies, offset_by):
        used = int((tallies > 0).sum())
        fixed = max(1, used // 4)
        shifted = fixed + (places - fixed + offset_by * (used - fixed)) % max(1, number_of - fixed)
        return jnp.zeros((number_of,), jnp.int32).at[order[jnp.where(places < fixed, places, shifted)]].set(jnp.asarray(tallies, jnp.int32))

    tallies = jnp.where(number % 4 == 0, named(heavy_load, number // 4), named(ordinary, number - number // 4 - 1))
    mixed = jax.random.permutation(jax.random.fold_in(own, 3), number_of)
    source_of, sink = mixed[0:number_of // 2 * 2:2], mixed[1:number_of // 2 * 2:2]
    margin = jnp.minimum(tallies[source_of] - 1, limit - tallies[sink]) // 2
    margin = jnp.where((source_of == order[0]) | (sink == order[0]) | (tallies[sink] == 0), 0, jnp.maximum(margin, 0))
    shifted = jax.random.randint(jax.random.fold_in(own, 4), (number_of // 2,), 0, 1 << 20) % (margin + 1)
    tallies = tallies.at[source_of].add(-shifted).at[sink].add(shifted)
    members = jnp.searchsorted(jnp.cumsum(tallies), jnp.arange(rows * top), side="right").astype(jnp.int32)
    table = members.reshape(top, rows).T
    table = table[jax.random.permutation(jax.random.fold_in(own, 1), rows)]
    offset_by = jax.random.randint(jax.random.fold_in(own, 2), (rows, 1), 0, top)
    return jnp.take_along_axis(table, (jnp.arange(top)[None, :] + offset_by) % top, axis=1)


def shares(count, total, most, skew, full):
    weights = [(1 << 20) // math.isqrt(grade ** skew) + 1 for grade in range(1, count + 1)]
    largest = most if full else min(most, max(-(-total // count), total * weights[0] // sum(weights)))
    least = 1 if total - largest >= count - 1 else 0
    given, rest = [largest] + [least] * (count - 1), total - largest - least * (count - 1)
    while rest > 0:
        candidates = [i for i in range(1, count) if given[i] < largest] or [i for i in range(1, count) if given[i] < most]
        mass, remaining = sum([weights[i] for i in candidates]), rest
        for i in candidates:
            extra = min(most - given[i], max(1, remaining * weights[i] // mass), rest)
            given[i] = given[i] + extra
            rest = rest - extra
    return np.array(given)


def scatter_about(own_key, dims, deviation, reach, shards=(), kind=jnp.bfloat16):
    entries = deviation * jax.random.normal(own_key, dims, jnp.float32)
    if shards:
        entries = entries * block_levels(own_key, dims, shards, -0.22, 0.18)
    return jnp.clip(entries, -reach, reach).astype(kind)


def setup_inputs(seed: int = 0) -> dict:
    keys = jax.random.split(jax.random.key(seed), 13)
    tokens = scatter_about(keys[0], (TOKENS, D), 1.0, 6.0, ((0, 8), (1, 4)))
    out_grad = scatter_about(keys[1], (TOKENS, D), 1.0, 6.0, ((0, 8), (1, 4)))
    expert_ids_keys = jax.random.split(jax.random.fold_in(keys[2], 1), TOKENS // TOK_DEV)
    expert_ids_turns = jax.random.permutation(jax.random.fold_in(keys[2], 3), TOKENS // TOK_DEV)
    expert_ids = jax.vmap(lambda own, number: routed_block(jax.random.fold_in(keys[2], 2), own, number, TOK_DEV, EXPERTS, TOP, CAP, 2))(expert_ids_keys, expert_ids_turns).reshape((TOKENS, TOP))
    tenant_ids = touch_ends(jax.random.randint(keys[3], (TOKENS,), 0, TENANTS), jax.random.fold_in(keys[3], 1), 0, TENANTS - 1).astype(jnp.int32)
    router_logits = scatter_about(keys[4], (TOKENS, TOP), 1.5, 8.0, ((0, 8),), jnp.float32)
    gate_projection_weight = scatter_about(keys[5], (EXPERTS, D, FF), D ** -0.5, 0.078125, ((0, 4), (2, 8)))
    up_projection_weight = scatter_about(keys[6], (EXPERTS, D, FF), D ** -0.5, 0.078125, ((0, 4), (2, 8)))
    down_projection_weight = scatter_about(keys[7], (EXPERTS, FF, D), FF ** -0.5, 0.0625, ((0, 4), (1, 8)))
    input_down_maps = scatter_about(keys[8], (EXPERTS, D, 2 * TENANT_RANKS), D ** -0.5, 0.078125, ((0, 4), (1, 4)))
    input_up_maps = scatter_about(keys[9], (EXPERTS, 2, TENANT_RANKS, FF), RANK ** -0.5, 1.5, ((0, 4), (3, 8)))
    output_down_map = scatter_about(keys[10], (EXPERTS, FF, TENANT_RANKS), FF ** -0.5, 0.0625, ((0, 4), (1, 8)))
    output_up_map = scatter_about(keys[11], (EXPERTS, TENANT_RANKS, D), RANK ** -0.5, 1.5, ((0, 4), (2, 4)))
    return {"tokens": tokens, "out_grad": out_grad, "expert_ids": expert_ids, "tenant_ids": tenant_ids, "router_logits": router_logits, "gate_projection_weight": gate_projection_weight, "up_projection_weight": up_projection_weight, "down_projection_weight": down_projection_weight, "input_down_maps": input_down_maps, "input_up_maps": input_up_maps, "output_down_map": output_down_map, "output_up_map": output_up_map}


ADAPTER_SCALE = 0.5


def matrix_product(left, right):
    return jnp.dot(left, right, preferred_element_type=jnp.float32)


def slot_rows(expert_ids):
    blocked = expert_ids.reshape(-1, TOK_DEV * TOP)
    labels = jnp.arange(EXPERTS, dtype=jnp.int32)
    onehot = (blocked[:, :, None] == labels[None, None, :]).astype(jnp.int32)
    before = jnp.cumsum(onehot, axis=1) - onehot
    position = jnp.sum(before * onehot, axis=2).astype(jnp.int32)
    block_index = jnp.arange(blocked.shape[0], dtype=jnp.int32)[:, None]
    return (block_index * CAP + position).reshape(-1, TOP).astype(jnp.int32)


def expert_step(inputs):
    (expert_token_rows, expert_gradients, exp_tenant, gate_matrix, up_matrix, down_matrix,
     expert_input_down, expert_input_up, expert_output_down, expert_output_up) = inputs
    columns = jnp.arange(TENANT_RANKS, dtype=jnp.int32) // RANK
    tenant_column_mask = (exp_tenant[:, None] == columns[None, :]).astype(jnp.float32)
    paired_mask = jnp.concatenate([tenant_column_mask, tenant_column_mask], axis=1)
    adapter_input = matrix_product(expert_token_rows, expert_input_down)
    adapter_rows = (paired_mask * adapter_input).astype(jnp.bfloat16)
    gate_activation = matrix_product(expert_token_rows, gate_matrix) + ADAPTER_SCALE * matrix_product(adapter_rows[:, :TENANT_RANKS], expert_input_up[0])
    up_activation = matrix_product(expert_token_rows, up_matrix) + ADAPTER_SCALE * matrix_product(adapter_rows[:, TENANT_RANKS:], expert_input_up[1])
    activated = jax.nn.silu(gate_activation)
    hidden_state = (activated * up_activation).astype(jnp.bfloat16)
    down_adapter_term = matrix_product(hidden_state, expert_output_down)
    down_row_values = (tenant_column_mask * down_adapter_term).astype(jnp.bfloat16)
    expert_output = (matrix_product(hidden_state, down_matrix) + ADAPTER_SCALE * matrix_product(down_row_values, expert_output_up)).astype(jnp.bfloat16)
    adapter_backward = matrix_product(expert_gradients, expert_output_up.T)
    backward_rows = (tenant_column_mask * adapter_backward).astype(jnp.bfloat16)
    hidden_gradient = matrix_product(expert_gradients, down_matrix.T) + ADAPTER_SCALE * matrix_product(backward_rows, expert_output_down.T)
    output_down_gradient = ADAPTER_SCALE * matrix_product(hidden_state.T, backward_rows)
    output_up_gradient = ADAPTER_SCALE * matrix_product(down_row_values.T, expert_gradients)
    sigmoid_gate = jax.nn.sigmoid(gate_activation)
    gate_gradient = (hidden_gradient * up_activation * sigmoid_gate * (1.0 + gate_activation * (1.0 - sigmoid_gate))).astype(jnp.bfloat16)
    up_gradient = (hidden_gradient * activated).astype(jnp.bfloat16)
    input_up_gradient = ADAPTER_SCALE * jnp.stack([matrix_product(adapter_rows[:, :TENANT_RANKS].T, gate_gradient), matrix_product(adapter_rows[:, TENANT_RANKS:].T, up_gradient)])
    up_adapter_term = jnp.concatenate([matrix_product(gate_gradient, expert_input_up[0].T), matrix_product(up_gradient, expert_input_up[1].T)], axis=1)
    up_row_values = (paired_mask * up_adapter_term).astype(jnp.bfloat16)
    input_down_gradient = ADAPTER_SCALE * matrix_product(expert_token_rows.T, up_row_values)
    running_partial_sum = matrix_product(gate_gradient, gate_matrix.T) + matrix_product(up_gradient, up_matrix.T)
    input_result = (running_partial_sum + ADAPTER_SCALE * matrix_product(up_row_values, expert_input_down.T)).astype(jnp.bfloat16)
    return expert_output, input_result, input_down_gradient, input_up_gradient, output_down_gradient, output_up_gradient


def reference(tokens, out_grad, expert_ids, tenant_ids, router_logits, gate_projection_weight, up_projection_weight, down_projection_weight, input_down_maps, input_up_maps, output_down_map, output_up_map):
    slot_index = slot_rows(expert_ids)
    flat_index = (expert_ids * ROWS + slot_index).reshape(-1).astype(jnp.int32)
    prob_first = jax.nn.sigmoid(router_logits[:, 0] - router_logits[:, 1])
    gate_probs = jnp.stack([prob_first, 1.0 - prob_first], axis=1)
    total_rows = EXPERTS * ROWS
    token_copies = jnp.repeat(tokens, TOP, axis=0)
    grad_copies = (gate_probs[:, :, None] * out_grad.astype(jnp.float32)[:, None, :]).astype(jnp.bfloat16).reshape(-1, D)
    tenant_copies = jnp.repeat(tenant_ids, TOP).astype(jnp.int32)
    expert_token_rows = jnp.zeros((total_rows, D), jnp.bfloat16).at[flat_index].set(token_copies)
    expert_gradients = jnp.zeros((total_rows, D), jnp.bfloat16).at[flat_index].set(grad_copies)
    exp_tenant = jnp.full((total_rows,), -1, jnp.int32).at[flat_index].set(tenant_copies)
    results = lax.map(expert_step, (expert_token_rows.reshape(EXPERTS, ROWS, D), expert_gradients.reshape(EXPERTS, ROWS, D),
                                    exp_tenant.reshape(EXPERTS, ROWS), gate_projection_weight, up_projection_weight, down_projection_weight, input_down_maps, input_up_maps, output_down_map, output_up_map))
    expert_output, input_result, input_down_gradient, input_up_gradient, output_down_gradient, output_up_gradient = results
    out_picked = expert_output.reshape(total_rows, D).astype(jnp.float32)[flat_index].reshape(-1, TOP, D)
    mixed = jnp.sum(gate_probs[:, :, None] * out_picked, axis=1).astype(jnp.bfloat16)
    grad_picked = input_result.reshape(total_rows, D).astype(jnp.float32)[flat_index].reshape(-1, TOP, D)
    input_grad = jnp.sum(grad_picked, axis=1).astype(jnp.bfloat16)
    return mixed, input_grad, input_down_gradient, input_up_gradient, output_down_gradient, output_up_gradient
```

```python
import functools

import jax
import jax.numpy as jnp
from jax import lax
from jax.experimental import pallas as pl
from jax.experimental.pallas import tpu as pltpu
from jax.sharding import PartitionSpec as P

RANK = 16
SCALE = 0.5
F32 = jnp.float32
BF16 = jnp.bfloat16
HIGH = lax.Precision.HIGHEST


def dot(a, b, dims=((1,), (0,)), precision=None):
    return lax.dot_general(
        a, b, (dims, ((), ())), preferred_element_type=F32, precision=precision
    )


def dot_nt(a, b, precision=None):
    return dot(a, b, ((1,), (1,)), precision)


def dot_tn(a, b):
    return dot(a, b, ((0,), (0,)))


def flip(index, mask):
    bit = 1
    while bit <= mask:
        if mask & bit:
            index = index + bit - 2 * bit * ((index // bit) % 2)
        bit *= 2
    return index


def bits_of(size):
    assert size & (size - 1) == 0
    return [1 << i for i in range(size.bit_length() - 1)]


def combos(bits):
    out = [0]
    for b in bits:
        out = out + [m | b for m in out]
    return out


def layer_kernel(
    nd, ne, nf,
    src, msk, wts, wg_hbm, wu_hbm, wd_hbm, idm, iup, odm, oum,
    mixed, igrad, idg, iug, odg, oug,
    gath, masks, xb, yb, wg, wu, wd, gate, up, hid, dgr, dur,
    q_s, vq_s, qz_s, wq_s, back, home,
    ar1s, ar1r, ar2s, ar2r, *rest,
):
    fbits, dbits = bits_of(nf), bits_of(nd)
    n_rs = len(fbits) + len(dbits)
    yr, xr = rest[:n_rs], rest[n_rs : 2 * n_rs]
    wsem, lsem, ssem, rsem = rest[2 * n_rs :]
    d, e, f = lax.axis_index("dp"), lax.axis_index("expert"), lax.axis_index("ffn")
    quarter = src.shape[2]
    hidden = wg.shape[2]
    rows_d = ne * 8
    rows = nd * rows_d
    cw = min(256, hidden)
    n_hc = hidden // cw
    qw = 256 if quarter % 256 == 0 else 128
    n_qc = quarter // qw
    pending = []
    counter = [0]

    def send(s, t, dev):
        i = counter[0]
        counter[0] += 1
        c = pltpu.make_async_remote_copy(
            src_ref=s, dst_ref=t, send_sem=ssem.at[i], recv_sem=rsem.at[i],
            device_id=dev, device_id_type=pl.DeviceIdType.MESH,
        )
        c.start()
        pending.append(c)
        return c

    arrival = [0]
    for b in reversed(fbits):
        arrival = arrival + [m | b for m in arrival]
    wcopies = []
    k = 0
    for m in arrival:
        qq = flip(f, m)
        pair = []
        for hbm, v in ((wg_hbm, wg), (wu_hbm, wu)):
            c = pltpu.make_async_copy(
                hbm.at[0, pl.ds(pl.multiple_of(qq * quarter, 128), quarter), :],
                v.at[qq], wsem.at[k],
            )
            c.start()
            k += 1
            pair.append(c)
        wcopies.append(pair)
    wd_copy = pltpu.make_async_copy(wd_hbm.at[0], wd, wsem.at[k])
    wd_copy.start()

    own = [
        pltpu.make_async_copy(src.at[e], gath.at[f, d, e], lsem.at[0]),
        pltpu.make_async_copy(msk.at[e], masks.at[d, e], lsem.at[1]),
    ]
    for c in own:
        c.start()

    barrier = pltpu.get_barrier_semaphore()
    peers = [(d, (e + j) % ne, f) for j in range(1, ne)]
    peers += [(flip(d, b), e, f) for b in dbits]
    peers += [(d, e, flip(f, b)) for b in fbits]
    for p in peers:
        pl.semaphore_signal(barrier, inc=1, device_id=p, device_id_type=pl.DeviceIdType.MESH)
    pl.semaphore_wait(barrier, len(peers))

    got = []
    for j in range(1, ne):
        to = (e + j) % ne
        got.append(send(src.at[to], gath.at[f, d, e], (d, to, f)))
        got.append(send(msk.at[to], masks.at[d, e], (d, to, f)))
    for c in own:
        c.wait()
    for c in got:
        c.wait_recv()

    top = fbits[-1] if fbits else 0
    early = []
    if top:
        early.append(send(gath.at[f, d], gath.at[f, d], (d, e, flip(f, top))))
    held = [0]
    for b in dbits:
        got = []
        for m in held:
            dm = flip(d, m)
            got.append(send(gath.at[f, dm], gath.at[f, dm], (flip(d, b), e, f)))
            got.append(send(masks.at[dm], masks.at[dm], (flip(d, b), e, f)))
        for c in got:
            c.wait_recv()
        if top:
            for m in held:
                dm = flip(d, b | m)
                early.append(send(gath.at[f, dm], gath.at[f, dm], (d, e, flip(f, top))))
        held = held + [m | b for m in held]

    half = ne // 2
    ys, xs = gath.at[:, :, :half], gath.at[:, :, half:]

    def unpack(q):
        def body(p, carry):
            dd, ee = p // half, (p % half) * 2
            v0 = gath[q, dd, ee].astype(F32)
            v1 = gath[q, dd, ee + 1].astype(F32)
            at = pl.ds(pl.multiple_of(p * 16, 16), 16)
            xb[q, at, :] = jnp.concatenate([v0[:8], v1[:8]], axis=0).astype(BF16)
            yb[q, at, :] = jnp.concatenate([v0[8:], v1[8:]], axis=0).astype(BF16)
            return carry

        lax.fori_loop(0, nd * half, body, 0)

    mask = masks[...].reshape(rows, masks.shape[3])
    ntr = mask.shape[1]
    mask3 = jnp.concatenate([mask, mask, mask], axis=1)
    lanes = 128
    col = lax.broadcasted_iota(jnp.int32, (3 * ntr, lanes), 0)
    lane = lax.broadcasted_iota(jnp.int32, (3 * ntr, lanes), 1)
    select = ((col // ntr) * RANK + col % RANK == lane).astype(F32)

    def compress(v):
        return dot(v * mask3, select, precision=HIGH)

    def expand(v):
        return dot_nt(v, select, precision=HIGH) * mask3

    def all_reduce(v, axes, sbuf, rbuf):
        for i, (axis, b) in enumerate(axes):
            sbuf[i] = v
            dev = (d, e, flip(f, b)) if axis == "f" else (flip(d, b), e, f)
            c = send(sbuf.at[i], rbuf.at[i], dev)
            yield
            c.wait_recv()
            v = v + rbuf[i]
        yield v

    def finish(gen):
        v = None
        for v in gen:
            pass
        return v

    unpack(f)
    pv = jnp.concatenate([dot(xb[f], idm[0]), dot_nt(yb[f], oum[0])], axis=1)
    ar1 = all_reduce(compress(pv), [("f", b) for b in reversed(fbits)], ar1s, ar1r)
    next(ar1)

    def project(m, first):
        q = flip(f, m)
        wcopies[arrival.index(m)][0].wait()
        wcopies[arrival.index(m)][1].wait()

        def body(c, carry):
            at = pl.ds(pl.multiple_of(c * cw, cw), cw)
            x = xb[q]
            g = dot(x, wg[q, :, at])
            u = dot(x, wu[q, :, at])
            if first:
                gate[:, at] = g
                up[:, at] = u
            else:
                gate[:, at] += g
                up[:, at] += u
            return carry

        lax.fori_loop(0, n_hc, body, 0)

    project(0, True)
    ready = [0]
    for n, b in enumerate(reversed(fbits)):
        if n == 0:
            got = early
        else:
            got = []
            for m in ready:
                qm = flip(f, m)
                got.append(send(gath.at[qm], gath.at[qm], (d, e, flip(f, b))))
        for c in got:
            c.wait_recv()
        ready = ready + [m | b for m in ready]
        if n + 1 < len(fbits):
            continue
    v = finish(ar1)
    pv = expand(v)
    q_s[...] = pv[:, : 2 * ntr].astype(BF16)
    vq_s[...] = pv[:, 2 * ntr :].astype(BF16)
    for m in arrival[1:]:
        unpack(flip(f, m))
        project(m, False)

    def activate(c, carry):
        at = pl.ds(pl.multiple_of(c * cw, cw), cw)
        g = gate[:, at] + SCALE * dot(q_s[:, :ntr], iup[0, 0, :, at])
        u = up[:, at] + SCALE * dot(q_s[:, ntr:], iup[0, 1, :, at])
        gate[:, at] = g
        up[:, at] = u
        hid[:, at] = (g * jax.nn.sigmoid(g) * u).astype(BF16)
        return carry

    lax.fori_loop(0, n_hc, activate, 0)

    def reduce_scatter(slabs, rbufs, produce):
        rec = {}
        for i, b in enumerate(fbits):
            ms = combos(fbits[i + 1 :])
            for n, m in enumerate(ms):
                add(slabs, rec, rbufs, i, b | m, produce)
                q = flip(f, b | m)
                rec[(i, m)] = (send(slabs.at[q], rbufs[i].at[n], (d, e, flip(f, b))), n)
                yield
        add(slabs, rec, rbufs, len(fbits), 0, produce)
        yield
        drec = {}
        for i, b in enumerate(dbits):
            r = rbufs[len(fbits) + i]
            ms = combos(dbits[i + 1 :])
            for n, m in enumerate(ms):
                dm = flip(d, b | m)
                for j in range(i):
                    c, pos = drec[(j, b | m)]
                    c.wait_recv()
                    slabs[f, dm] = (
                        slabs[f, dm].astype(F32) + rbufs[len(fbits) + j][pos].astype(F32)
                    ).astype(BF16)
                drec[(i, m)] = (send(slabs.at[f, dm], r.at[n], (flip(d, b), e, f)), n)
        yield
        total = slabs[f, d].astype(F32)
        for i in range(len(dbits)):
            c, pos = drec[(i, 0)]
            c.wait_recv()
            total = total + rbufs[len(fbits) + i][pos].astype(F32)
        yield total.reshape(rows_d, quarter)

    def add(slabs, rec, rbufs, upto, m, produce):
        q = flip(f, m)
        produce(q)
        for j in range(upto):
            c, pos = rec[(j, m)]
            c.wait_recv()
            slabs[q] = (slabs[q].astype(F32) + rbufs[j][pos].astype(F32)).astype(BF16)

    wd_copy.wait()
    for c in pending:
        c.wait_send()
    pending.clear()

    def produce_y(q):
        def body(c, carry):
            at = pl.ds(pl.multiple_of(c * qw, qw), qw)
            v = dot(hid[...], wd[:, pl.ds(pl.multiple_of(q * quarter + c * qw, qw), qw)])
            ys[q, :, :, :, at] = v.astype(BF16).reshape(nd, half, 16, qw)
            return carry

        lax.fori_loop(0, n_qc, body, 0)

    def produce_x(q):
        def body(c, carry):
            at = pl.ds(pl.multiple_of(c * qw, qw), qw)
            v = dot_nt(dgr[...], wg[q, at, :]) + dot_nt(dur[...], wu[q, at, :])
            xs[q, :, :, :, at] = v.astype(BF16).reshape(nd, half, 16, qw)
            return carry

        lax.fori_loop(0, n_qc, body, 0)

    y_gen = reduce_scatter(ys, yr, produce_y)
    for _ in range(nf):
        next(y_gen)
    z = dot(hid[...], odm[0])

    def backward(c, carry):
        at = pl.ds(pl.multiple_of(c * cw, cw), cw)
        dh = SCALE * dot_nt(vq_s[...], odm[0, at, :])
        for q in range(nf):
            dh = dh + dot_nt(yb[q], wd[at, q * quarter : (q + 1) * quarter])
        g = gate[:, at]
        s = jax.nn.sigmoid(g)
        dgr[:, at] = (dh * up[:, at] * s * (1.0 + g * (1.0 - s))).astype(BF16)
        dur[:, at] = (dh * (g * s)).astype(BF16)
        return carry

    lax.fori_loop(0, n_hc, backward, 0)
    next(y_gen)
    w0 = dot_nt(dgr[...], iup[0, 0])
    w1 = dot_nt(dur[...], iup[0, 1])
    ar2 = all_reduce(
        compress(jnp.concatenate([z, w0, w1], axis=1)),
        [("f", b) for b in fbits] + [("d", b) for b in dbits], ar2s, ar2r,
    )
    next(ar2)
    x_gen = reduce_scatter(xs, xr, produce_x)
    zw = None
    for _ in range(nf):
        next(x_gen)
        if zw is None:
            zw = next(ar2)
    while zw is None:
        zw = next(ar2)
    next(x_gen)
    zw = expand(zw)
    qz_s[...] = zw[:, :ntr].astype(BF16)
    wq_s[...] = zw[:, ntr:].astype(BF16)

    mine = pl.ds(pl.multiple_of(d * rows_d, 16), rows_d)
    y_add = SCALE * dot(qz_s[mine, :], oum[0])
    x_add = SCALE * dot_nt(wq_s[mine, :], idm[0])
    y_own = next(y_gen) + y_add
    x_own = next(x_gen) + x_add
    for j in range(ne):
        at = slice(j * 8, j * 8 + 8)
        back[j] = jnp.concatenate([y_own[at], x_own[at]], axis=0).astype(BF16)
    home_own = pltpu.make_async_copy(back.at[e], home.at[e], lsem.at[2])
    home_own.start()
    got = []
    for j in range(1, ne):
        to = (e + j) % ne
        got.append(send(back.at[to], home.at[e], (d, to, f)))

    idg[0] = SCALE * dot_tn(xb[f], wq_s[...])
    oug[0] = SCALE * dot_tn(qz_s[...], yb[f])
    odg[0] = SCALE * dot_tn(hid[...], vq_s[...])
    iug[0, 0] = SCALE * dot_tn(q_s[:, :ntr], dgr[...])
    iug[0, 1] = SCALE * dot_tn(q_s[:, ntr:], dur[...])

    home_own.wait()
    for c in got:
        c.wait_recv()
    out = jnp.zeros((8, quarter), F32)
    grad = jnp.zeros((8, quarter), F32)
    for j in range(ne):
        v = home[j].astype(F32)
        out = out + wts[j, :, :1] * v[:8]
        grad = grad + v[8:]
    mixed[...] = out.astype(BF16)
    igrad[...] = grad.astype(BF16)
    for c in pending:
        c.wait_send()


def per_device(
    tokens, out_grad, expert_ids, tenant_ids, router_logits,
    gate_projection_weight, up_projection_weight, down_projection_weight,
    input_down_maps, input_up_maps, output_down_map, output_up_map,
):
    ne, nd, nf = lax.axis_size("expert"), lax.axis_size("dp"), lax.axis_size("ffn")
    tok, quarter = tokens.shape
    hidden = gate_projection_weight.shape[2]
    ntr = output_down_map.shape[2]
    rows_d = ne * tok
    rows = nd * rows_d
    first = jax.nn.sigmoid(router_logits[:, 0] - router_logits[:, 1])
    probs = jnp.stack([first, 1.0 - first], axis=1)
    hit = expert_ids[None] == jnp.arange(ne, dtype=jnp.int32)[:, None, None]
    member = jnp.any(hit, axis=2)
    weight = jnp.sum(jnp.where(hit, probs[None], 0.0), axis=2)
    x = jnp.where(member[:, :, None], tokens[None], jnp.zeros((), BF16))
    dy = (weight[:, :, None] * out_grad.astype(F32)[None]).astype(BF16)
    src = jnp.concatenate([x, dy], axis=1)
    column = jnp.arange(ntr, dtype=jnp.int32) // RANK
    msk = (member[:, :, None] & (tenant_ids[None, :, None] == column[None, None])).astype(F32)
    wts = jnp.broadcast_to(weight[:, :, None], (ne, tok, 128))

    fbits, dbits = bits_of(nf), bits_of(nd)
    rs_bufs = [pltpu.VMEM((nf >> (i + 1), nd, ne // 2, 16, quarter), BF16) for i in range(len(fbits))]
    rs_bufs += [pltpu.VMEM((nd >> (i + 1), ne // 2, 16, quarter), BF16) for i in range(len(dbits))]
    n_sem = (
        3 * (ne - 1) + 3 * nd + nf + 2 * (nf + nd) + 2 * len(fbits) + len(dbits)
    )
    n1, n2 = max(len(fbits), 1), max(len(fbits) + len(dbits), 1)
    vmem = pl.BlockSpec(memory_space=pltpu.VMEM)
    hbm = pl.BlockSpec(memory_space=pl.ANY)
    return pl.pallas_call(
        functools.partial(layer_kernel, nd, ne, nf),
        out_shape=(
            jax.ShapeDtypeStruct(tokens.shape, BF16),
            jax.ShapeDtypeStruct(tokens.shape, BF16),
            jax.ShapeDtypeStruct(input_down_maps.shape, F32),
            jax.ShapeDtypeStruct(input_up_maps.shape, F32),
            jax.ShapeDtypeStruct(output_down_map.shape, F32),
            jax.ShapeDtypeStruct(output_up_map.shape, F32),
        ),
        in_specs=[vmem] * 3 + [hbm] * 3 + [vmem] * 4,
        out_specs=[vmem] * 6,
        scratch_shapes=[
            pltpu.VMEM((nf, nd, ne, 2 * tok, quarter), BF16),
            pltpu.VMEM((nd, ne, tok, ntr), F32),
            pltpu.VMEM((nf, rows, quarter), BF16),
            pltpu.VMEM((nf, rows, quarter), BF16),
            pltpu.VMEM((nf, quarter, hidden), BF16),
            pltpu.VMEM((nf, quarter, hidden), BF16),
            pltpu.VMEM((hidden, nf * quarter), BF16),
            pltpu.VMEM((rows, hidden), F32),
            pltpu.VMEM((rows, hidden), F32),
            pltpu.VMEM((rows, hidden), BF16),
            pltpu.VMEM((rows, hidden), BF16),
            pltpu.VMEM((rows, hidden), BF16),
            pltpu.VMEM((rows, 2 * ntr), BF16),
            pltpu.VMEM((rows, ntr), BF16),
            pltpu.VMEM((rows, ntr), BF16),
            pltpu.VMEM((rows, 2 * ntr), BF16),
            pltpu.VMEM((ne, 2 * tok, quarter), BF16),
            pltpu.VMEM((ne, 2 * tok, quarter), BF16),
            pltpu.VMEM((n1, rows, 128), F32),
            pltpu.VMEM((n1, rows, 128), F32),
            pltpu.VMEM((n2, rows, 128), F32),
            pltpu.VMEM((n2, rows, 128), F32),
            *rs_bufs,
            *rs_bufs,
            pltpu.SemaphoreType.DMA((2 * nf + 1,)),
            pltpu.SemaphoreType.DMA((3,)),
            pltpu.SemaphoreType.DMA((n_sem,)),
            pltpu.SemaphoreType.DMA((n_sem,)),
        ],
        compiler_params=pltpu.CompilerParams(
            collective_id=0, has_side_effects=True, vmem_limit_bytes=67043328
        ),
    )(
        src, msk, wts,
        gate_projection_weight, up_projection_weight, down_projection_weight,
        input_down_maps, input_up_maps, output_down_map, output_up_map,
    )


def solution(mesh):
    return jax.shard_map(
        per_device,
        mesh=mesh,
        in_specs=(
            P(("dp", "expert"), "ffn"),
            P(("dp", "expert"), "ffn"),
            P(("dp", "expert"), None),
            P(("dp", "expert")),
            P(("dp", "expert"), None),
            P("expert", None, ("dp", "ffn")),
            P("expert", None, ("dp", "ffn")),
            P("expert", ("dp", "ffn"), None),
            P("expert", "ffn", None),
            P("expert", None, None, ("dp", "ffn")),
            P("expert", ("dp", "ffn"), None),
            P("expert", None, "ffn"),
        ),
        out_specs=(
            P(("dp", "expert"), "ffn"),
            P(("dp", "expert"), "ffn"),
            P("expert", "ffn", None),
            P("expert", None, None, ("dp", "ffn")),
            P("expert", ("dp", "ffn"), None),
            P("expert", None, "ffn"),
        ),
        check_vma=False,
    )
```
